32 devices in a mesh: rep: 1, r: 8 (over y, z), s: 4 (over x, core).
Axes of the slice: x: 2, y: 2, z: 4, core: 2. Of those that a mesh axis runs over, the one named last changes fastest.
Arguments:
- x: bfloat16 [32, 4096, 640], P(('rep', 'r', 's'))
- dy: bfloat16 [32, 4096, 640], P(('rep', 'r', 's'))
- w_gate: bfloat16 [2, 640, 2560], P(None, 's')
- w_up: bfloat16 [2, 640, 2560], P(None, 's')
- w_down: bfloat16 [2, 2560, 640], P(None, 's')
- m_w_gate: float32 [2, 640, 2560], P(None, 's')
- m_w_up: float32 [2, 640, 2560], P(None, 's')
- m_w_down: float32 [2, 2560, 640], P(None, 's')
- v_w_gate: float32 [2, 640, 2560], P(None, 's')
- v_w_up: float32 [2, 640, 2560], P(None, 's')
- v_w_down: float32 [2, 2560, 640], P(None, 's')
Outputs:
- output 1: bfloat16 [2, 640, 2560], P('rep', 's')
- output 2: bfloat16 [2, 640, 2560], P('rep', 's')
- output 3: bfloat16 [2, 2560, 640], P('rep', 's')
- output 4: float32 [2, 640, 2560], P('rep', 's')
- output 5: float32 [2, 640, 2560], P('rep', 's')
- output 6: float32 [2, 2560, 640], P('rep', 's')
- output 7: float32 [2, 640, 2560], P('rep', 's')
- output 8: float32 [2, 640, 2560], P('rep', 's')
- output 9: float32 [2, 2560, 640], P('rep', 's')
All inputs are finite; a program needn't handle non-finite values.
Results may differ from the reference program's by a relative error of at most 0.022.
Values are sent between devices in bfloat16 or wider.
A program may use at most 2 GiB of HBM per device.

```python
import jax
import jax.numpy as jnp
from jax import lax

SEQUENCES = 32
TOKENS = 4096
D = 640
FF = 2560
LAYERS = 2
NAMES = ("w_gate", "w_up", "w_down")
SHAPES = {"w_gate": (LAYERS, D, FF), "w_up": (LAYERS, D, FF), "w_down": (LAYERS, FF, D)}


def bump(key, n, height):
    away = (jnp.arange(n, dtype=jnp.int32) - jax.random.randint(key, (), 0, n, jnp.int32)) % n
    return jnp.where(away < n // 8, height, 1.0)


def together(key, own, strength):
    shared = jax.random.normal(key, own.shape[1:], jnp.float32)
    return (own + strength * shared) * lax.rsqrt(1 + strength * strength)


def setup_inputs(seed: int = 0, part: int = 0) -> dict:
    kx, kdy, ka, kb, kz, kf, kh, kl, *keys = jax.random.split(jax.random.key(seed), 8 + 3 * len(NAMES))
    kx, kdy, ka, kb = (jax.random.fold_in(k, part) for k in (kx, kdy, ka, kb))
    kw, km, kv = (keys[i::3] for i in range(3))
    shape = (SEQUENCES, TOKENS, D)
    much_x, much_dy = jax.random.uniform(kz, (2,), jnp.float32, 0.0, 1.0)
    loud = 2.0 ** jax.random.uniform(jax.random.fold_in(kz, 1), (), jnp.float32, -1.0, 2.0)
    layers = 2.0 ** jax.random.uniform(kl, (LAYERS, 1, 1), jnp.float32, -1.0, 1.0)
    x = together(ka, jax.random.normal(kx, shape, jnp.float32), much_x) * bump(kf, D, 4.0)
    dy = together(kb, jax.random.normal(kdy, shape, jnp.float32), much_dy)
    drawn = {"x": x.astype(jnp.bfloat16), "dy": (loud * dy * (SEQUENCES * TOKENS) ** -0.5).astype(jnp.bfloat16)}
    for key, name in zip(kw, NAMES, strict=True):
        w = jax.random.normal(key, SHAPES[name], jnp.float32) * SHAPES[name][1] ** -0.5
        drawn[name] = (w * {"w_gate": 1.0, "w_up": bump(kh, FF, 4.0), "w_down": layers}[name]).astype(jnp.bfloat16)
    for key, name in zip(km, NAMES, strict=True):
        drawn[f"m_{name}"] = 0.1 * jax.random.normal(key, SHAPES[name], jnp.float32)
    for key, name in zip(kv, NAMES, strict=True):
        drawn[f"v_{name}"] = jax.random.uniform(key, SHAPES[name], jnp.float32, 0.005, 0.015)
    return drawn


def matmul(a, w):
    return jnp.dot(a, w, preferred_element_type=jnp.float32).astype(jnp.bfloat16)


def normed(h):
    wide = h.astype(jnp.float32)
    scale = lax.rsqrt(jnp.mean(wide**2, -1, keepdims=True) + 1e-6)
    return (wide * scale).astype(jnp.bfloat16)


def layer(h, w):
    a = normed(h)
    gate = jnp.dot(a, w["w_gate"], preferred_element_type=jnp.float32)
    up = jnp.dot(a, w["w_up"], preferred_element_type=jnp.float32)
    return h + matmul((jax.nn.silu(gate) * up).astype(jnp.bfloat16), w["w_down"])


def adamw(w, m, v, g):
    m = 0.9 * m + 0.1 * g
    v = 0.95 * v + 0.05 * g * g
    step = m * lax.rsqrt(v + 1e-8) + 0.1 * w
    return (w - 0.02 * step).astype(jnp.bfloat16), m, v


def stack(weights, h):
    return lax.scan(lambda h, w: (layer(h, w), None), h, weights)[0]


def reference(x, dy, w_gate, w_up, w_down, m_w_gate, m_w_up, m_w_down, v_w_gate, v_w_up, v_w_down):
    weights = dict(zip(NAMES, (w_gate, w_up, w_down), strict=True))

    def take(so_far, sequence):
        h, by_y = sequence
        _, back = jax.vjp(lambda w: stack(w, h), weights)
        return jax.tree.map(lambda total, term: total + term.astype(jnp.float32), so_far, back(by_y)[0]), None

    none_yet = {name: jnp.zeros(w.shape, jnp.float32) for name, w in weights.items()}
    by_weights, _ = lax.scan(take, none_yet, (x, dy))
    gradients = [by_weights[name].astype(jnp.bfloat16).astype(jnp.float32) for name in NAMES]
    new = [
        adamw(w.astype(jnp.float32), m, v, g)
        for w, m, v, g in zip((w_gate, w_up, w_down), (m_w_gate, m_w_up, m_w_down), (v_w_gate, v_w_up, v_w_down), gradients, strict=True)
    ]
    return tuple(one[which] for which in range(3) for one in new)
```

```python
import functools

import jax
import jax.numpy as jnp
from jax import lax
from jax.experimental import pallas as pl
from jax.experimental.pallas import tpu as pltpu
from jax.sharding import PartitionSpec as P

BF, F32 = jnp.bfloat16, jnp.float32
NN = (((1,), (0,)), ((), ()))
NT = (((1,), (1,)), ((), ()))
MESH = pl.DeviceIdType.MESH
ANY = pl.BlockSpec(memory_space=pl.ANY)
DMA = pltpu.SemaphoreType.DMA
VMEM_LIMIT = 67_000_000
CHUNKS, STEPS, TILE, SUB = 5, 4, 1024, 512


def dot(a, b, dims=NN):
    return lax.dot_general(a, b, dims, preferred_element_type=F32)


def normed(h):
    wide = h.astype(F32)
    return wide, lax.rsqrt(jnp.mean(wide * wide, -1, keepdims=True) + 1e-6)


def place():
    r, s = lax.axis_index("r"), lax.axis_index("s")
    x, core = s // 2, lax.rem(s, 2)
    return r, x, r // 4, core, lax.rem(r + 4, 8), lax.rem(s + 2, 4), s + 1 - 2 * core


def unpack(w_ref, wg, wu, wd):
    rows, width = w_ref.shape[2] // 3, w_ref.shape[3]
    part = width // 4
    for s in range(4):
        wg[s * rows : (s + 1) * rows, :] = w_ref[s // 2, s % 2, 0:rows, :]
        wu[s * rows : (s + 1) * rows, :] = w_ref[s // 2, s % 2, rows : 2 * rows, :]
        for k in range(4):
            wd[k * rows : (k + 1) * rows, s * part : (s + 1) * part] = w_ref[s // 2, s % 2, 2 * rows :, k * part : (k + 1) * part]


def pack(p_ref, dg, du, dd):
    rows, width = p_ref.shape[2] // 3, p_ref.shape[3]
    part = width // 4
    for s in range(4):
        p_ref[s // 2, s % 2, 0:rows, :] = dg[s * rows : (s + 1) * rows, :].astype(BF)
        p_ref[s // 2, s % 2, rows : 2 * rows, :] = du[s * rows : (s + 1) * rows, :].astype(BF)
        for k in range(4):
            p_ref[s // 2, s % 2, 2 * rows :, k * part : (k + 1) * part] = dd[k * rows : (k + 1) * rows, s * part : (s + 1) * part].astype(BF)


def remote(src, dst, send, recv, **to):
    return pltpu.make_async_remote_copy(src_ref=src, dst_ref=dst, send_sem=send, recv_sem=recv, device_id=to, device_id_type=MESH)


def forward_kernel(g_ref, u_ref, d_ref, x_ref, w_ref, h_ref, gate_ref, up_ref, a_s, out_s, wg, wu, wd, own, wbuf, keep, fetch, send, recv):
    j, t = pl.program_id(0), pl.program_id(1)
    step = j * STEPS + t
    _, x, y, core, other_y, other_x, other_core = place()
    count = 2 * CHUNKS
    half = own.shape[1] // 2
    mine, theirs = pl.ds(y * half, half), pl.ds((1 - y) * half, half)

    def over_core(k):
        return remote(own.at[k], w_ref.at[k, x, core], send.at[0, k], recv.at[0, k], s=other_core)

    def over_x(k):
        return remote(own.at[k, mine], w_ref.at[k, x, core, mine], send.at[1, k], recv.at[1, k], s=other_x)

    def over_y(k):
        at = w_ref.at[k, 1 - x, core, mine]
        return remote(at, at, send.at[2, k], recv.at[2, k], r=other_y)

    def on_first(k):
        at = w_ref.at[k, 1 - x, core, mine]
        return remote(at, at, send.at[3, k], recv.at[3, k], s=other_core)

    def on_second(k):
        at = w_ref.at[k, 1 - x, core, theirs]
        return remote(at, at, send.at[4, k], recv.at[4, k], s=other_core)

    def kept(k):
        return pltpu.make_async_copy(own.at[k], w_ref.at[k, x, core], keep.at[k])

    def fetched(k, slot):
        return pltpu.make_async_copy(w_ref.at[k], wbuf.at[slot], fetch.at[slot])

    def from_x(k):
        over_x(k).wait_recv()
        over_y(k).start()
        on_first(k).start()

    def from_y(k):
        over_y(k).wait_recv()
        on_second(k).start()

    def whole(k):
        for copy in (over_core, on_first, on_second):
            copy(k).wait_recv()
        kept(k).wait()

    @pl.when(step == 0)
    def _():
        barrier = pltpu.get_barrier_semaphore()
        for to in ({"s": other_core}, {"s": other_x}, {"r": other_y}):
            pl.semaphore_signal(barrier, inc=1, device_id=to, device_id_type=MESH)
        rows, part = own.shape[1] // 3, own.shape[2] // 4
        for layer in range(2):
            down = d_ref[layer].T
            for chunk in range(CHUNKS):
                k = layer * CHUNKS + chunk
                for q in range(4):
                    to = slice(q * part, (q + 1) * part)
                    at = slice((q * CHUNKS + chunk) * part, (q * CHUNKS + chunk + 1) * part)
                    own[k, 0:rows, to] = g_ref[layer, :, at]
                    own[k, rows : 2 * rows, to] = u_ref[layer, :, at]
                    own[k, 2 * rows :, to] = down[q * rows : (q + 1) * rows, chunk * part : (chunk + 1) * part]
        pl.semaphore_wait(barrier, 3)

        @pl.loop(0, count)
        def _(k):
            over_x(k).start()
            over_core(k).start()
            kept(k).start()

        from_x(0)
        from_x(1)
        from_y(0)
        whole(0)
        fetched(0, 0).start()

    @pl.when((lax.rem(step, 2) == 1) & (step < 2 * count - 4))
    def _():
        from_x((step + 3) // 2)

    @pl.when((lax.rem(step, 2) == 1) & (step < 2 * count - 2))
    def _():
        from_y((step + 1) // 2)

    @pl.when((lax.rem(step, 2) == 0) & (step > 0))
    def _():
        whole(step // 2)

    @pl.when(t == 0)
    def _():
        slot = lax.rem(j, 2)
        fetched(j, slot).wait()
        unpack(wbuf.at[slot], wg, wu, wd)

    @pl.when((t == STEPS - 1) & (j < CHUNKS - 1))
    def _():
        fetched(j + 1, lax.rem(j + 1, 2)).start()

    @pl.when(j == 0)
    def _():
        wide, scale = normed(x_ref[...])
        a_s[t] = (wide * scale).astype(BF)
        out_s[t] = jnp.zeros_like(out_s[t])

    for i in range(TILE // SUB):
        at = slice(i * SUB, (i + 1) * SUB)
        a = a_s[t, at, :]
        gate, up = dot(a, wg[...]), dot(a, wu[...])
        gate_ref[0, at, :] = gate
        up_ref[0, at, :] = up
        hidden = (gate * jax.nn.sigmoid(gate) * up).astype(BF)
        out_s[t, :, at] += dot(wd[...], hidden, NT)

    @pl.when(j == CHUNKS - 1)
    def _():
        h_ref[...] = x_ref[...] + out_s[t].astype(BF).T

    @pl.when(step == CHUNKS * STEPS - 1)
    def _():
        @pl.loop(0, count)
        def _(k):
            for copy in (over_core, over_x, over_y, on_first, on_second):
                copy(k).wait_send()


class Sum:
    def __init__(self, p_ref, g_ref, y_s, r1, r2, z_s, ry, rz, g_s, load, keep, send, recv):
        self.p, self.g, self.y_s, self.r1, self.r2, self.z_s, self.ry, self.rz, self.g_s = p_ref, g_ref, y_s, r1, r2, z_s, ry, rz, g_s
        self.load, self.keep, self.send, self.recv = load, keep, send, recv
        self.r, self.x, self.y, self.core, self.other_y, self.other_x, self.other_core = place()
        self.z = lax.rem(self.r, 4)

    @staticmethod
    def scratch(rows, width):
        piece = (rows // 2, width // 4)
        return [
            pltpu.VMEM((2, 2, rows, width), BF),
            pltpu.VMEM((CHUNKS, 2, rows, width), BF),
            pltpu.VMEM((CHUNKS, rows, width), BF),
            pltpu.VMEM((CHUNKS, 8) + piece, BF),
            pltpu.VMEM((CHUNKS, 4) + piece, BF),
            pltpu.VMEM((CHUNKS, 4) + piece, BF),
            pltpu.VMEM((CHUNKS, 8) + piece, BF),
            DMA((2,)),
            DMA((CHUNKS,)),
            DMA((CHUNKS, 10)),
            DMA((CHUNKS, 10)),
        ]

    def over_core(self, k):
        return remote(self.p.at[k, :, 1 - self.core], self.r1.at[k], self.send.at[k, 0], self.recv.at[k, 0], s=self.other_core)

    def loaded(self, k):
        return pltpu.make_async_copy(self.p.at[k, :, self.core], self.y_s.at[k % 2], self.load.at[k % 2])

    def over_x(self, k):
        return remote(self.y_s.at[k % 2, 1 - self.x], self.r2.at[k], self.send.at[k, 1], self.recv.at[k, 1], s=self.other_x)

    def over_y(self, k):
        return remote(self.z_s.at[k, pl.ds(4 * (1 - self.y), 4)], self.ry.at[k], self.send.at[k, 2], self.recv.at[k, 2], r=self.other_y)

    def over_z(self, k, d):
        to = lax.rem(self.z + d, 4)
        return remote(self.z_s.at[k, 4 * self.y + to], self.rz.at[k, self.z], self.send.at[k, 2 + d], self.recv.at[k, 2 + d], r=4 * self.y + to)

    def back_z(self, k, d):
        at = self.g_s.at[k, self.r]
        return remote(at, at, self.send.at[k, 5 + d], self.recv.at[k, 5 + d], r=4 * self.y + lax.rem(self.z + d, 4))

    def back_y(self, k):
        at = self.g_s.at[k, pl.ds(4 * self.y, 4)]
        return remote(at, at, self.send.at[k, 9], self.recv.at[k, 9], r=self.other_y)

    def kept(self, k):
        return pltpu.make_async_copy(self.g_s.at[k], self.g.at[k], self.keep.at[k])

    def greet(self):
        barrier = pltpu.get_barrier_semaphore()
        others = [{"r": 4 * self.y + lax.rem(self.z + d, 4)} for d in range(1, 4)]
        for to in [{"s": self.other_core}, {"s": self.other_x}, {"r": self.other_y}] + others:
            pl.semaphore_signal(barrier, inc=1, device_id=to, device_id_type=MESH)
        pl.semaphore_wait(barrier, 6)

    def start(self):
        for k in range(CHUNKS):
            self.over_core(k).start()
        for k in range(2):
            self.loaded(k).start()

    def add_core(self, k):
        self.loaded(k).wait()
        self.over_core(k).wait_recv()
        self.y_s[k % 2] = (self.y_s[k % 2].astype(F32) + self.r1[k].astype(F32)).astype(BF)
        self.over_x(k).start()

    def add_x(self, k):
        self.over_x(k).wait_recv()
        high, wide = self.z_s.shape[2:]
        for piece in range(8):
            at = (slice(piece // 4 * high, (piece // 4 + 1) * high), slice(piece % 4 * wide, (piece % 4 + 1) * wide))
            self.z_s[k, piece] = (self.y_s[(k % 2, self.x) + at].astype(F32) + self.r2[(k,) + at].astype(F32)).astype(BF)
        self.over_y(k).start()
        self.over_x(k).wait_send()
        if k + 2 < CHUNKS:
            self.loaded(k + 2).start()

    def add_y(self, k):
        self.over_y(k).wait_recv()
        mine = pl.ds(4 * self.y, 4)
        self.z_s[k, mine] = (self.z_s[k, mine].astype(F32) + self.ry[k].astype(F32)).astype(BF)
        for d in range(1, 4):
            self.over_z(k, d).start()

    def add_z(self, k):
        total = self.z_s[k, self.r].astype(F32)
        for d in range(1, 4):
            self.over_z(k, d).wait_recv()
        for d in range(1, 4):
            total += self.rz[k, lax.rem(self.z + d, 4)].astype(F32)
        self.g_s[k, self.r] = total.astype(BF)
        for d in range(1, 4):
            self.back_z(k, d).start()

    def gather_y(self, k):
        for d in range(1, 4):
            self.back_z(k, d).wait_recv()
        self.back_y(k).start()

    def finish(self, k):
        self.back_y(k).wait_recv()
        self.kept(k).start()

    def sent(self):
        for k in range(CHUNKS):
            self.kept(k).wait()
            self.over_core(k).wait_send()
            self.over_y(k).wait_send()
            self.back_y(k).wait_send()
            for d in range(1, 4):
                self.over_z(k, d).wait_send()
                self.back_z(k, d).wait_send()


def sum_kernel(p_ref, g_ref, *scratch):
    total = Sum(p_ref, g_ref, *scratch)
    total.greet()
    total.start()
    total.add_core(0)
    total.add_core(1)
    for n in range(CHUNKS + 4):
        if n < CHUNKS:
            total.add_x(n)
            if n + 2 < CHUNKS:
                total.add_core(n + 2)
        for late, stage in enumerate((total.add_y, total.add_z, total.gather_y, total.finish)):
            if 0 <= n - late < CHUNKS:
                stage(n - late)
    total.sent()


def backward_kernel(first, h_ref, dy_ref, w_ref, *refs):
    if first:
        gate_ref, up_ref, q_ref, p_ref, g_ref, at_s, dyt_s, dg_s, du_s, dd_s, wg, wu, wd, *scratch = refs
    else:
        p_ref, dh_ref, at_s, dyt_s, dg_s, du_s, dd_s, wg, wu, wd, a_s, da_s = refs
    j, t = pl.program_id(0), pl.program_id(1)

    if first:
        total = Sum(q_ref, g_ref, *scratch)
        stages = {0: [total.greet, total.start]}
        for k in range(CHUNKS):
            for stage, at in ((total.add_core, 1), (total.add_x, 4), (total.add_y, 6), (total.add_z, 8), (total.gather_y, 10), (total.finish, 12)):
                stages.setdefault(min(at + 3 * k, CHUNKS * STEPS - 1), []).append(functools.partial(stage, k))
        stages[CHUNKS * STEPS - 1].append(total.sent)
        for at, todo in sorted(stages.items()):

            @pl.when(j * STEPS + t == at)
            def _(todo=todo):
                for one in todo:
                    one()

    @pl.when(t == 0)
    def _():
        unpack(w_ref.at[0], wg, wu, wd)
        for s in (dg_s, du_s, dd_s):
            s[...] = jnp.zeros_like(s)

    @pl.when(j == 0)
    def _():
        wide, scale = normed(h_ref[...])
        a = (wide * scale).astype(BF)
        at_s[t] = a.T
        dyt_s[t] = dy_ref[...].T
        if not first:
            a_s[t] = a
            da_s[t] = jnp.zeros_like(da_s[t])

    for i in range(TILE // SUB):
        at = slice(i * SUB, (i + 1) * SUB)
        if first:
            gate, up = gate_ref[0, at, :], up_ref[0, at, :]
        else:
            a = a_s[t, at, :]
            gate, up = dot(a, wg[...]), dot(a, wu[...])
        by_hidden = dot(dy_ref[at, :], wd[...]).astype(BF).astype(F32)
        sig = jax.nn.sigmoid(gate)
        silu = gate * sig
        hidden = (silu * up).astype(BF)
        by_up = (by_hidden * silu).astype(BF)
        by_gate = (by_hidden * up * (sig + silu * (1.0 - sig))).astype(BF)
        dd_s[...] += dot(dyt_s[t, :, at], hidden)
        du_s[...] += dot(at_s[t, :, at], by_up)
        dg_s[...] += dot(at_s[t, :, at], by_gate)
        if not first:
            da_s[t, :, at] += dot(wg[...], by_gate, NT) + dot(wu[...], by_up, NT)

    @pl.when(t == STEPS - 1)
    def _():
        pack(p_ref.at[0], dg_s, du_s, dd_s)

    if not first:

        @pl.when(j == CHUNKS - 1)
        def _():
            wide, scale = normed(h_ref[...])
            da = da_s[t].astype(BF).T.astype(F32)
            inner = jnp.mean(da * wide, -1, keepdims=True)
            dh_ref[...] = dy_ref[...] + (da * scale - wide * (scale * scale * scale * inner)).astype(BF)


def adamw(w, m, v, g):
    g = g.astype(F32)
    m = 0.9 * m + 0.1 * g
    v = 0.95 * v + 0.05 * g * g
    step = m * lax.rsqrt(v + 1e-8) + 0.1 * w.astype(F32)
    return (w.astype(F32) - 0.02 * step).astype(BF), m, v


def columns_kernel(below, above, *refs):
    rows = refs[0].shape[1]
    part = below.shape[-1]

    def take(g):
        for chunk in range(CHUNKS):
            at = slice(chunk * part, (chunk + 1) * part)
            both = jnp.concatenate([g[chunk, 0, 0], g[chunk, 1, 0, : 2 * rows - g.shape[3]]], 0)
            for i in range(2):
                w, m, v = (refs[3 * i + k][0, :, at] for k in range(3))
                new = adamw(w, m, v, both[i * rows : (i + 1) * rows])
                for k in range(3):
                    refs[6 + 3 * i + k][0, :, at] = new[k]

    @pl.when(pl.program_id(0) == 0)
    def _():
        take(below)

    @pl.when(pl.program_id(0) == 1)
    def _():
        take(above)


def rows_kernel(below, above, w, m, v, *outs):
    def take(g):
        rows = w.shape[2] // 4
        skip = g.shape[3] - rows
        turned = jnp.concatenate([g[0, 0, q, skip:] for q in range(4)], 0).T
        for out, new in zip(outs, adamw(w[0], m[0], v[0], turned), strict=True):
            out[0] = new

    @pl.when(pl.program_id(0) == 0)
    def _():
        take(below)

    @pl.when(pl.program_id(0) == 1)
    def _():
        take(above)


def solution(mesh):
    def step(x, dy, *arrays):
        x, dy = x[0], dy[0]
        weights, m, v = (arrays[i : i + 3] for i in (0, 3, 6))
        tokens, d = x.shape
        layers, rows, ff = weights[0].shape
        width, deep = ff // CHUNKS, 3 * rows
        part = width // 4
        shape = jax.ShapeDtypeStruct

        def params(flops, **more):
            return dict(
                compiler_params=pltpu.CompilerParams(vmem_limit_bytes=VMEM_LIMIT, **more),
                cost_estimate=pl.CostEstimate(flops=flops * tokens * d * ff, bytes_accessed=0, transcendentals=0),
            )

        tok = pl.BlockSpec((TILE, d), lambda j, t: (t, 0))
        late = pl.BlockSpec((TILE, d), lambda j, t: (jnp.where(j == CHUNKS - 1, t, 0), 0))
        saved = pl.BlockSpec((1, TILE, width), lambda j, t: (j, t, 0))
        package = pl.BlockSpec((1, 2, 2, deep, width), lambda j, t: (j, 0, 0, 0, 0))
        above = pl.BlockSpec((1, 2, 2, deep, width), lambda j, t: (CHUNKS + j, 0, 0, 0, 0))
        packages = shape((CHUNKS, 2, 2, deep, width), BF)
        grads = shape((CHUNKS, 8, deep // 2, part), BF)
        matrices = [pltpu.VMEM((d, width), BF)] * 3
        across = [pltpu.VMEM((STEPS, d, TILE), BF)] * 2
        sums = [pltpu.VMEM((d, width), F32)] * 3
        count = layers * CHUNKS

        w, h, gate, up = pl.pallas_call(
            forward_kernel,
            grid=(CHUNKS, STEPS),
            in_specs=[pl.BlockSpec(w.shape, lambda j, t: (0, 0, 0), pipeline_mode=pl.Buffered(1)) for w in weights] + [tok],
            out_specs=[ANY, late, saved, saved],
            out_shape=[shape((count, 2, 2, deep, width), BF), shape(x.shape, BF)] + [shape((CHUNKS, tokens, width), F32)] * 2,
            scratch_shapes=[pltpu.VMEM((STEPS, TILE, d), BF), pltpu.VMEM((STEPS, d, TILE), F32)]
            + matrices
            + [pltpu.VMEM((count, deep, width), BF), pltpu.VMEM((2, 2, 2, deep, width), BF)]
            + [DMA((count,)), DMA((2,)), DMA((5, count)), DMA((5, count))],
            name="forward",
            **params(6, collective_id=0, has_side_effects=True),
        )(*weights, x)
        above_grads, dh = pl.pallas_call(
            functools.partial(backward_kernel, False),
            grid=(CHUNKS, STEPS),
            in_specs=[tok, tok, above],
            out_specs=[package, late],
            out_shape=[packages, shape(x.shape, BF)],
            scratch_shapes=across + sums + matrices + [pltpu.VMEM((STEPS, TILE, d), BF), pltpu.VMEM((STEPS, d, TILE), F32)],
            name="backward_1",
            **params(16),
        )(h, dy, w)
        below_grads, above_sum = pl.pallas_call(
            functools.partial(backward_kernel, True),
            grid=(CHUNKS, STEPS),
            in_specs=[tok, tok, package, saved, saved, ANY],
            out_specs=[package, ANY],
            out_shape=[packages, grads],
            scratch_shapes=across + sums + matrices + Sum.scratch(deep, width),
            name="backward_0",
            **params(8, collective_id=1, has_side_effects=True),
        )(x, dh, w, gate, up, above_grads)
        below_sum = pl.pallas_call(
            sum_kernel,
            in_specs=[ANY],
            out_specs=ANY,
            out_shape=grads,
            scratch_shapes=Sum.scratch(deep, width),
            name="last_sum",
            **params(1, collective_id=2, has_side_effects=True),
        )(below_grads)

        g = [total.reshape(CHUNKS, 2, 4, deep // 2, part) for total in (below_sum, above_sum)]
        block = pl.BlockSpec((1, rows, CHUNKS * part), lambda layer, s: (layer, 0, s))
        both = pl.BlockSpec((CHUNKS, 2, 1, deep // 2, part), lambda layer, s: (0, 0, s, 0, 0))
        new = pl.pallas_call(
            columns_kernel,
            grid=(layers, 4),
            in_specs=[both] * 2 + [block] * 6,
            out_specs=[block] * 6,
            out_shape=[shape((layers, rows, ff), t) for t in (BF, F32, F32)] * 2,
            name="columns",
            **params(1),
        )(*g, weights[0], m[0], v[0], weights[1], m[1], v[1])
        block = pl.BlockSpec((1, part, d), lambda layer, j: (layer, j, 0))
        both = pl.BlockSpec((1, 1, 4, deep // 2, part), lambda layer, j: (j, 1, 0, 0, 0))
        new += pl.pallas_call(
            rows_kernel,
            grid=(layers, CHUNKS),
            in_specs=[both] * 2 + [block] * 3,
            out_specs=[block] * 3,
            out_shape=[shape((layers, CHUNKS * part, d), t) for t in (BF, F32, F32)],
            name="rows",
            **params(1),
        )(*g, weights[2], m[2], v[2])
        return tuple(new[3 * i + k] for k in range(3) for i in range(3))

    states, cut = P(("rep", "r", "s"), None, None), P(None, "s", None)
    return jax.shard_map(step, mesh=mesh, in_specs=(states, states) + (cut,) * 9, out_specs=(P("rep", "s", None),) * 9, check_vma=False)
```

```python
import functools

import jax
import jax.numpy as jnp
from jax import lax
from jax.experimental import pallas as pl
from jax.experimental.pallas import tpu as pltpu
from jax.sharding import PartitionSpec as P

BF, F32 = jnp.bfloat16, jnp.float32
NN = (((1,), (0,)), ((), ()))
NT = (((1,), (1,)), ((), ()))
MESH = pl.DeviceIdType.MESH
ANY = pl.BlockSpec(memory_space=pl.ANY)
DMA = pltpu.SemaphoreType.DMA
VMEM_LIMIT = 67_000_000
CHUNKS, STEPS, TILE, SUB, WIDE = 5, 4, 1024, 512, 1024


def dot(a, b, dims=NN):
    return lax.dot_general(a, b, dims, preferred_element_type=F32)


def normed(h):
    wide = h.astype(F32)
    return wide, lax.rsqrt(jnp.mean(wide * wide, -1, keepdims=True) + 1e-6)


def place():
    r, s = lax.axis_index("r"), lax.axis_index("s")
    x, core = s // 2, lax.rem(s, 2)
    return r, x, r // 4, core, lax.rem(r + 4, 8), lax.rem(s + 2, 4), s + 1 - 2 * core


def unpack(w_ref, wg, wu, wd):
    rows, width = w_ref.shape[2] // 3, w_ref.shape[3]
    part = width // 4
    for s in range(4):
        wg[s * rows : (s + 1) * rows, :] = w_ref[s // 2, s % 2, 0:rows, :]
        wu[s * rows : (s + 1) * rows, :] = w_ref[s // 2, s % 2, rows : 2 * rows, :]
        for k in range(4):
            wd[k * rows : (k + 1) * rows, s * part : (s + 1) * part] = w_ref[s // 2, s % 2, 2 * rows :, k * part : (k + 1) * part]


def pack(p_ref, dg, du, dd):
    rows, width = p_ref.shape[2] // 3, p_ref.shape[3]
    part = width // 4
    for s in range(4):
        p_ref[s // 2, s % 2, 0:rows, :] = dg[s * rows : (s + 1) * rows, :].astype(BF)
        p_ref[s // 2, s % 2, rows : 2 * rows, :] = du[s * rows : (s + 1) * rows, :].astype(BF)
        for k in range(4):
            p_ref[s // 2, s % 2, 2 * rows :, k * part : (k + 1) * part] = dd[k * rows : (k + 1) * rows, s * part : (s + 1) * part].astype(BF)


def remote(src, dst, send, recv, **to):
    return pltpu.make_async_remote_copy(src_ref=src, dst_ref=dst, send_sem=send, recv_sem=recv, device_id=to, device_id_type=MESH)


def forward_kernel(g_ref, u_ref, d_ref, x_ref, w_ref, h_ref, gate_ref, up_ref, a_s, out_s, wg, wu, wd, own, wbuf, keep, fetch, send, recv):
    j, t = pl.program_id(0), pl.program_id(1)
    step = j * STEPS + t
    _, x, y, core, other_y, other_x, other_core = place()
    count = 2 * CHUNKS
    half = own.shape[1] // 2
    mine, theirs = pl.ds(y * half, half), pl.ds((1 - y) * half, half)

    def over_core(k):
        return remote(own.at[k], w_ref.at[k, x, core], send.at[0, k], recv.at[0, k], s=other_core)

    def over_x(k):
        return remote(own.at[k, mine], w_ref.at[k, x, core, mine], send.at[1, k], recv.at[1, k], s=other_x)

    def over_y(k):
        at = w_ref.at[k, 1 - x, core, mine]
        return remote(at, at, send.at[2, k], recv.at[2, k], r=other_y)

    def on_first(k):
        at = w_ref.at[k, 1 - x, core, mine]
        return remote(at, at, send.at[3, k], recv.at[3, k], s=other_core)

    def on_second(k):
        at = w_ref.at[k, 1 - x, core, theirs]
        return remote(at, at, send.at[4, k], recv.at[4, k], s=other_core)

    def kept(k):
        return pltpu.make_async_copy(own.at[k], w_ref.at[k, x, core], keep.at[k])

    def fetched(k, slot):
        return pltpu.make_async_copy(w_ref.at[k], wbuf.at[slot], fetch.at[slot])

    def from_x(k):
        over_x(k).wait_recv()
        over_y(k).start()
        on_first(k).start()

    def from_y(k):
        over_y(k).wait_recv()
        on_second(k).start()

    def whole(k):
        for copy in (over_core, on_first, on_second):
            copy(k).wait_recv()
        kept(k).wait()

    @pl.when(step == 0)
    def _():
        barrier = pltpu.get_barrier_semaphore()
        for to in ({"s": other_core}, {"s": other_x}, {"r": other_y}):
            pl.semaphore_signal(barrier, inc=1, device_id=to, device_id_type=MESH)
        rows, part = own.shape[1] // 3, own.shape[2] // 4
        for layer in range(2):
            down = d_ref[layer].T
            for chunk in range(CHUNKS):
                k = layer * CHUNKS + chunk
                for q in range(4):
                    to = slice(q * part, (q + 1) * part)
                    at = slice((q * CHUNKS + chunk) * part, (q * CHUNKS + chunk + 1) * part)
                    own[k, 0:rows, to] = g_ref[layer, :, at]
                    own[k, rows : 2 * rows, to] = u_ref[layer, :, at]
                    own[k, 2 * rows :, to] = down[q * rows : (q + 1) * rows, chunk * part : (chunk + 1) * part]
        pl.semaphore_wait(barrier, 3)

        @pl.loop(0, count)
        def _(k):
            over_x(k).start()
            over_core(k).start()
            kept(k).start()

        from_x(0)
        from_x(1)
        from_y(0)
        whole(0)
        fetched(0, 0).start()

    @pl.when((lax.rem(step, 2) == 1) & (step < 2 * count - 4))
    def _():
        from_x((step + 3) // 2)

    @pl.when((lax.rem(step, 2) == 1) & (step < 2 * count - 2))
    def _():
        from_y((step + 1) // 2)

    @pl.when((lax.rem(step, 2) == 0) & (step > 0))
    def _():
        whole(step // 2)

    @pl.when(t == 0)
    def _():
        slot = lax.rem(j, 2)
        fetched(j, slot).wait()
        unpack(wbuf.at[slot], wg, wu, wd)

    @pl.when((t == STEPS - 1) & (j < CHUNKS - 1))
    def _():
        fetched(j + 1, lax.rem(j + 1, 2)).start()

    @pl.when(j == 0)
    def _():
        wide, scale = normed(x_ref[...])
        a_s[t] = (wide * scale).astype(BF)
        out_s[t] = jnp.zeros_like(out_s[t])

    for i in range(TILE // WIDE):
        at = slice(i * WIDE, (i + 1) * WIDE)
        a = a_s[t, at, :]
        gate, up = dot(a, wg[...]), dot(a, wu[...])
        gate_ref[0, at, :] = gate
        up_ref[0, at, :] = up
        hidden = (gate * jax.nn.sigmoid(gate) * up).astype(BF)
        out_s[t, :, at] += dot(wd[...], hidden, NT)

    @pl.when(j == CHUNKS - 1)
    def _():
        h_ref[...] = x_ref[...] + out_s[t].astype(BF).T

    @pl.when(step == CHUNKS * STEPS - 1)
    def _():
        @pl.loop(0, count)
        def _(k):
            for copy in (over_core, over_x, over_y, on_first, on_second):
                copy(k).wait_send()


class Sum:
    def __init__(self, count, g_ref, p_s, r1, r2, z_s, ry, rz, g_s, keep, send, recv, credit):
        self.count, self.slots = count, p_s.shape[0]
        self.g, self.p_s, self.r1, self.r2, self.z_s, self.ry, self.rz, self.g_s = g_ref, p_s, r1, r2, z_s, ry, rz, g_s
        self.keep, self.send, self.recv, self.credit = keep, send, recv, credit
        self.r, self.x, self.y, self.core, self.other_y, self.other_x, self.other_core = place()
        self.z = lax.rem(self.r, 4)
        self.partners = [({"s": self.other_core}, 0), ({"s": self.other_x}, 1), ({"r": self.other_y}, 2)]
        self.partners += [({"r": self.along_z(d)}, 6 - d) for d in range(1, 4)]

    @staticmethod
    def scratch(slots, rows, width):
        piece = (rows // 2, width // 4)
        return [
            pltpu.VMEM((slots, 2, 2, rows, width), BF),
            pltpu.VMEM((slots, 2, rows, width), BF),
            pltpu.VMEM((slots, rows, width), BF),
            pltpu.VMEM((slots, 8) + piece, BF),
            pltpu.VMEM((slots, 4) + piece, BF),
            pltpu.VMEM((slots, 4) + piece, BF),
            pltpu.VMEM((slots, 8) + piece, BF),
            DMA((slots,)),
            DMA((slots, 10)),
            DMA((slots, 10)),
            pltpu.SemaphoreType.REGULAR((6,)),
        ]

    def along_z(self, d):
        return 4 * self.y + lax.rem(self.z + d, 4)

    def copy(self, src, dst, k, which, **to):
        return remote(src, dst, self.send.at[k % self.slots, which], self.recv.at[k % self.slots, which], **to)

    def over_core(self, k):
        n = k % self.slots
        return self.copy(self.p_s.at[n, :, 1 - self.core], self.r1.at[n], k, 0, s=self.other_core)

    def over_x(self, k):
        n = k % self.slots
        return self.copy(self.p_s.at[n, 1 - self.x, self.core], self.r2.at[n], k, 1, s=self.other_x)

    def over_y(self, k):
        n = k % self.slots
        return self.copy(self.z_s.at[n, pl.ds(4 * (1 - self.y), 4)], self.ry.at[n], k, 2, r=self.other_y)

    def over_z(self, k, d):
        n = k % self.slots
        return self.copy(self.z_s.at[n, self.along_z(d)], self.rz.at[n, self.z], k, 2 + d, r=self.along_z(d))

    def back_z(self, k, d):
        at = self.g_s.at[k % self.slots, self.r]
        return self.copy(at, at, k, 5 + d, r=self.along_z(d))

    def back_y(self, k):
        at = self.g_s.at[k % self.slots, pl.ds(4 * self.y, 4)]
        return self.copy(at, at, k, 9, r=self.other_y)

    def kept(self, k):
        return pltpu.make_async_copy(self.g_s.at[k % self.slots], self.g.at[k], self.keep.at[k % self.slots])

    def greet(self):
        barrier = pltpu.get_barrier_semaphore()
        for to, _ in self.partners:
            pl.semaphore_signal(barrier, inc=1, device_id=to, device_id_type=MESH)
        pl.semaphore_wait(barrier, 6)

    def begin(self, k):
        if k >= self.slots:
            for i in range(6):
                pl.semaphore_wait(self.credit.at[i], 1)
        self.over_core(k).start()

    def add_core(self, k):
        n = k % self.slots
        self.over_core(k).wait_recv()
        for x in range(2):
            self.p_s[n, x, self.core] = (self.p_s[n, x, self.core].astype(F32) + self.r1[n, x].astype(F32)).astype(BF)
        self.over_x(k).start()

    def add_x(self, k):
        n = k % self.slots
        self.over_x(k).wait_recv()
        high, wide = self.z_s.shape[2:]
        for piece in range(8):
            at = (slice(piece // 4 * high, (piece // 4 + 1) * high), slice(piece % 4 * wide, (piece % 4 + 1) * wide))
            self.z_s[n, piece] = (self.p_s[(n, self.x, self.core) + at].astype(F32) + self.r2[(n,) + at].astype(F32)).astype(BF)
        self.over_y(k).start()

    def add_y(self, k):
        n = k % self.slots
        self.over_y(k).wait_recv()
        mine = pl.ds(4 * self.y, 4)
        self.z_s[n, mine] = (self.z_s[n, mine].astype(F32) + self.ry[n].astype(F32)).astype(BF)
        for d in range(1, 4):
            self.over_z(k, d).start()

    def add_z(self, k):
        n = k % self.slots
        total = self.z_s[n, self.r].astype(F32)
        for d in range(1, 4):
            self.over_z(k, d).wait_recv()
        for d in range(1, 4):
            total += self.rz[n, lax.rem(self.z + d, 4)].astype(F32)
        self.g_s[n, self.r] = total.astype(BF)
        for d in range(1, 4):
            self.back_z(k, d).start()

    def gather_y(self, k):
        for d in range(1, 4):
            self.back_z(k, d).wait_recv()
        self.back_y(k).start()

    def finish(self, k):
        self.back_y(k).wait_recv()
        self.kept(k).start()
        for copy in (self.over_core, self.over_x, self.over_y, self.back_y):
            copy(k).wait_send()
        for d in range(1, 4):
            self.over_z(k, d).wait_send()
            self.back_z(k, d).wait_send()

    def release(self, k):
        self.kept(k).wait()
        if k + self.slots < self.count:
            for to, i in self.partners:
                pl.semaphore_signal(self.credit.at[i], inc=1, device_id=to, device_id_type=MESH)

    def timed(self, begins, after):
        stages = (self.begin, self.add_core, self.add_x, self.add_y, self.add_z, self.gather_y, self.finish, self.release)
        return [(at + late, functools.partial(stage, k)) for k, at in enumerate(begins) for stage, late in zip(stages, (0,) + after, strict=True)]


EARLY = 3


def run_at(step, timed, last):
    timed = sorted(timed, key=lambda one: one[0])
    for at in sorted({one[0] for one in timed if one[0] <= last}):

        @pl.when(step == at)
        def _(at=at):
            for when, what in timed:
                if when == at:
                    what()

    return [what for when, what in timed if when > last]


def backward_kernel(first, h_ref, dy_ref, w_ref, *refs):
    if first:
        gate_ref, up_ref, q_ref, g_ref, at_s, dyt_s, dg_s, du_s, dd_s, wg, wu, wd, *scratch, load = refs
        total = Sum(2 * CHUNKS - EARLY, g_ref, *scratch)
    else:
        g_ref, q_ref, dh_ref, at_s, dyt_s, dg_s, du_s, dd_s, wg, wu, wd, a_s, da_s, *scratch, load = refs
        total = Sum(EARLY, g_ref, *scratch)
    j, t = pl.program_id(0), pl.program_id(1)
    step, last = j * STEPS + t, CHUNKS * STEPS - 1
    p_s, slots = total.p_s, total.slots

    if first:

        def taken(i):
            return pltpu.make_async_copy(q_ref.at[i], p_s.at[i], load.at[i])

        timed = [(0, taken(i).start) for i in range(CHUNKS - EARLY)] + [(0, total.greet)]
        timed += [(3 * i, taken(i).wait) for i in range(CHUNKS - EARLY)]
        timed += total.timed((0, 3, 6, 9, 12, 16, last + 0.9), (1, 4, 6, 8, 10, 11, 12))
        ahead = CHUNKS - EARLY
    else:

        def taken(i):
            return pltpu.make_async_copy(p_s.at[(EARLY + i) % slots], q_ref.at[i], load.at[i])

        timed = [(0, total.greet)] + total.timed((4, 8, 12), (1, 3, 4, 5, 6, 7, 7))
        timed += [(STEPS * (EARLY + i + 1), taken(i).start) for i in range(CHUNKS - EARLY)]
        timed += [(last + 2, taken(i).wait) for i in range(CHUNKS - EARLY)]
        ahead = 0
    rest = run_at(step, timed, last)

    @pl.when(t == 0)
    def _():
        unpack(w_ref.at[0], wg, wu, wd)
        for s in (dg_s, du_s, dd_s):
            s[...] = jnp.zeros_like(s)

    @pl.when(j == 0)
    def _():
        wide, scale = normed(h_ref[...])
        a = (wide * scale).astype(BF)
        at_s[t] = a.T
        dyt_s[t] = dy_ref[...].T
        if not first:
            a_s[t] = a
            da_s[t] = jnp.zeros_like(da_s[t])

    for i in range(TILE // SUB):
        at = slice(i * SUB, (i + 1) * SUB)
        if first:
            gate, up = gate_ref[0, at, :], up_ref[0, at, :]
        else:
            a = a_s[t, at, :]
            gate, up = dot(a, wg[...]), dot(a, wu[...])
        by_hidden = dot(dy_ref[at, :], wd[...]).astype(BF).astype(F32)
        sig = jax.nn.sigmoid(gate)
        silu = gate * sig
        hidden = (silu * up).astype(BF)
        by_up = (by_hidden * silu).astype(BF)
        by_gate = (by_hidden * up * (sig + silu * (1.0 - sig))).astype(BF)
        dd_s[...] += dot(dyt_s[t, :, at], hidden)
        du_s[...] += dot(at_s[t, :, at], by_up)
        dg_s[...] += dot(at_s[t, :, at], by_gate)
        if not first:
            da_s[t, :, at] += dot(wg[...], by_gate, NT) + dot(wu[...], by_up, NT)

    @pl.when(t == STEPS - 1)
    def _():
        pack(p_s.at[lax.rem(j + ahead, slots)], dg_s, du_s, dd_s)

    if not first:

        @pl.when(j == CHUNKS - 1)
        def _():
            wide, scale = normed(h_ref[...])
            da = da_s[t].astype(BF).T.astype(F32)
            inner = jnp.mean(da * wide, -1, keepdims=True)
            dh_ref[...] = dy_ref[...] + (da * scale - wide * (scale * scale * scale * inner)).astype(BF)

    @pl.when(step == last)
    def _():
        for what in rest:
            what()


def adamw(w, m, v, g):
    g = g.astype(F32)
    m = 0.9 * m + 0.1 * g
    v = 0.95 * v + 0.05 * g * g
    step = m * lax.rsqrt(v + 1e-8) + 0.1 * w.astype(F32)
    return (w.astype(F32) - 0.02 * step).astype(BF), m, v


def columns_kernel(early, late, *refs):
    rows = refs[0].shape[1]
    part = early.shape[-1]

    def take(chunks):
        for chunk, (g, n) in enumerate(chunks):
            at = slice(chunk * part, (chunk + 1) * part)
            both = jnp.concatenate([g[n, 0, 0], g[n, 1, 0, : 2 * rows - g.shape[3]]], 0)
            for i in range(2):
                w, m, v = (refs[3 * i + k][0, :, at] for k in range(3))
                new = adamw(w, m, v, both[i * rows : (i + 1) * rows])
                for k in range(3):
                    refs[6 + 3 * i + k][0, :, at] = new[k]

    @pl.when(pl.program_id(0) == 0)
    def _():
        take([(late, CHUNKS - EARLY + n) for n in range(CHUNKS)])

    @pl.when(pl.program_id(0) == 1)
    def _():
        take([(early, n) for n in range(EARLY)] + [(late, n) for n in range(CHUNKS - EARLY)])


def rows_kernel(early, late, w, m, v, *outs):
    def take(g):
        rows = w.shape[2] // 4
        skip = g.shape[3] - rows
        turned = jnp.concatenate([g[0, 0, q, skip:] for q in range(4)], 0).T
        for out, new in zip(outs, adamw(w[0], m[0], v[0], turned), strict=True):
            out[0] = new

    from_early = (pl.program_id(0) == 1) & (pl.program_id(1) < EARLY)

    @pl.when(from_early)
    def _():
        take(early)

    @pl.when(jnp.logical_not(from_early))
    def _():
        take(late)


def solution(mesh):
    def step(x, dy, *arrays):
        x, dy = x[0], dy[0]
        weights, m, v = (arrays[i : i + 3] for i in (0, 3, 6))
        tokens, d = x.shape
        layers, rows, ff = weights[0].shape
        width, deep = ff // CHUNKS, 3 * rows
        part = width // 4
        shape = jax.ShapeDtypeStruct

        def params(flops, **more):
            return dict(
                compiler_params=pltpu.CompilerParams(vmem_limit_bytes=VMEM_LIMIT, **more),
                cost_estimate=pl.CostEstimate(flops=flops * tokens * d * ff, bytes_accessed=0, transcendentals=0),
            )

        tok = pl.BlockSpec((TILE, d), lambda j, t: (t, 0))
        late = pl.BlockSpec((TILE, d), lambda j, t: (jnp.where(j == CHUNKS - 1, t, 0), 0))
        saved = pl.BlockSpec((1, TILE, width), lambda j, t: (j, t, 0))
        package = pl.BlockSpec((1, 2, 2, deep, width), lambda j, t: (j, 0, 0, 0, 0))
        above = pl.BlockSpec((1, 2, 2, deep, width), lambda j, t: (CHUNKS + j, 0, 0, 0, 0))
        packages = shape((CHUNKS - EARLY, 2, 2, deep, width), BF)
        grads = [shape((n, 8, deep // 2, part), BF) for n in (EARLY, 2 * CHUNKS - EARLY)]
        matrices = [pltpu.VMEM((d, width), BF)] * 3
        across = [pltpu.VMEM((STEPS, d, TILE), BF)] * 2
        sums = [pltpu.VMEM((d, width), F32)] * 3
        count = layers * CHUNKS

        w, h, gate, up = pl.pallas_call(
            forward_kernel,
            grid=(CHUNKS, STEPS),
            in_specs=[pl.BlockSpec(w.shape, lambda j, t: (0, 0, 0), pipeline_mode=pl.Buffered(1)) for w in weights] + [tok],
            out_specs=[ANY, late, saved, saved],
            out_shape=[shape((count, 2, 2, deep, width), BF), shape(x.shape, BF)] + [shape((CHUNKS, tokens, width), F32)] * 2,
            scratch_shapes=[pltpu.VMEM((STEPS, TILE, d), BF), pltpu.VMEM((STEPS, d, TILE), F32)]
            + matrices
            + [pltpu.VMEM((count, deep, width), BF), pltpu.VMEM((2, 2, 2, deep, width), BF)]
            + [DMA((count,)), DMA((2,)), DMA((5, count)), DMA((5, count))],
            name="forward",
            **params(6, collective_id=0, has_side_effects=True),
        )(*weights, x)
        early, waiting, dh = pl.pallas_call(
            functools.partial(backward_kernel, False),
            grid=(CHUNKS, STEPS),
            in_specs=[tok, tok, above],
            out_specs=[ANY, ANY, late],
            out_shape=[grads[0], packages, shape(x.shape, BF)],
            scratch_shapes=across + sums + matrices + [pltpu.VMEM((STEPS, TILE, d), BF), pltpu.VMEM((STEPS, d, TILE), F32)] + Sum.scratch(2, deep, width) + [DMA((2,))],
            name="backward_1",
            **params(16, collective_id=1, has_side_effects=True),
        )(h, dy, w)
        rest = pl.pallas_call(
            functools.partial(backward_kernel, True),
            grid=(CHUNKS, STEPS),
            in_specs=[tok, tok, package, saved, saved, ANY],
            out_specs=ANY,
            out_shape=grads[1],
            scratch_shapes=across + sums + matrices + Sum.scratch(4, deep, width) + [DMA((2,))],
            name="backward_0",
            **params(8, collective_id=2, has_side_effects=True),
        )(x, dh, w, gate, up, waiting)

        g = [total.reshape(-1, 2, 4, deep // 2, part) for total in (early, rest)]
        block = pl.BlockSpec((1, rows, CHUNKS * part), lambda layer, s: (layer, 0, s))
        both = [pl.BlockSpec((total.shape[0], 2, 1, deep // 2, part), lambda layer, s: (0, 0, s, 0, 0)) for total in g]
        new = pl.pallas_call(
            columns_kernel,
            grid=(layers, 4),
            in_specs=both + [block] * 6,
            out_specs=[block] * 6,
            out_shape=[shape((layers, rows, ff), t) for t in (BF, F32, F32)] * 2,
            name="columns",
            **params(1),
        )(*g, weights[0], m[0], v[0], weights[1], m[1], v[1])
        block = pl.BlockSpec((1, part, d), lambda layer, j: (layer, j, 0))
        both = [
            pl.BlockSpec((1, 1, 4, deep // 2, part), lambda layer, j: (jnp.minimum(j, EARLY - 1), 1, 0, 0, 0)),
            pl.BlockSpec((1, 1, 4, deep // 2, part), lambda layer, j: (jnp.where(layer == 0, j + CHUNKS - EARLY, jnp.maximum(j - EARLY, 0)), 1, 0, 0, 0)),
        ]
        new += pl.pallas_call(
            rows_kernel,
            grid=(layers, CHUNKS),
            in_specs=both + [block] * 3,
            out_specs=[block] * 3,
            out_shape=[shape((layers, CHUNKS * part, d), t) for t in (BF, F32, F32)],
            name="rows",
            **params(1),
        )(*g, weights[2], m[2], v[2])
        return tuple(new[3 * i + k] for k in range(3) for i in range(3))

    states, cut = P(("rep", "r", "s"), None, None), P(None, "s", None)
    return jax.shard_map(step, mesh=mesh, in_specs=(states, states) + (cut,) * 9, out_specs=(P("rep", "s", None),) * 9, check_vma=False)
```

```python
import functools

import jax
import jax.numpy as jnp
from jax import lax
from jax.experimental import pallas as pl
from jax.experimental.pallas import tpu as pltpu
from jax.sharding import PartitionSpec as P

BF, F32 = jnp.bfloat16, jnp.float32
NN = (((1,), (0,)), ((), ()))
NT = (((1,), (1,)), ((), ()))
MESH = pl.DeviceIdType.MESH
ANY = pl.BlockSpec(memory_space=pl.ANY)
DMA = pltpu.SemaphoreType.DMA
VMEM_LIMIT = 67_000_000
CHUNKS, STEPS, TILE, SUB, WIDE = 5, 4, 1024, 512, 1024


def dot(a, b, dims=NN):
    return lax.dot_general(a, b, dims, preferred_element_type=F32)


def normed(h):
    wide = h.astype(F32)
    return wide, lax.rsqrt(jnp.mean(wide * wide, -1, keepdims=True) + 1e-6)


def place():
    r, s = lax.axis_index("r"), lax.axis_index("s")
    x, core = s // 2, lax.rem(s, 2)
    return r, x, r // 4, core, lax.rem(r + 4, 8), lax.rem(s + 2, 4), s + 1 - 2 * core


def unpack(w_ref, wg, wu, wd):
    rows, width = w_ref.shape[2] // 3, w_ref.shape[3]
    part = width // 4
    for s in range(4):
        wg[s * rows : (s + 1) * rows, :] = w_ref[s // 2, s % 2, 0:rows, :]
        wu[s * rows : (s + 1) * rows, :] = w_ref[s // 2, s % 2, rows : 2 * rows, :]
        for k in range(4):
            wd[k * rows : (k + 1) * rows, s * part : (s + 1) * part] = w_ref[s // 2, s % 2, 2 * rows :, k * part : (k + 1) * part]


def pack(p_ref, dg, du, dd):
    rows, width = p_ref.shape[2] // 3, p_ref.shape[3]
    part = width // 4
    for s in range(4):
        p_ref[s // 2, s % 2, 0:rows, :] = dg[s * rows : (s + 1) * rows, :].astype(BF)
        p_ref[s // 2, s % 2, rows : 2 * rows, :] = du[s * rows : (s + 1) * rows, :].astype(BF)
        for k in range(4):
            p_ref[s // 2, s % 2, 2 * rows :, k * part : (k + 1) * part] = dd[k * rows : (k + 1) * rows, s * part : (s + 1) * part].astype(BF)


def remote(src, dst, send, recv, **to):
    return pltpu.make_async_remote_copy(src_ref=src, dst_ref=dst, send_sem=send, recv_sem=recv, device_id=to, device_id_type=MESH)


def forward_kernel(g_ref, u_ref, d_ref, x_ref, w_ref, h_ref, gate_ref, up_ref, a_s, out_s, wg, wu, wd, own, wbuf, keep, fetch, send, recv):
    j, t = pl.program_id(0), pl.program_id(1)
    step = j * STEPS + t
    _, x, y, core, other_y, other_x, other_core = place()
    count = 2 * CHUNKS
    half = own.shape[1] // 2
    mine, theirs = pl.ds(y * half, half), pl.ds((1 - y) * half, half)

    def over_core(k):
        return remote(own.at[k], w_ref.at[k, x, core], send.at[0, k], recv.at[0, k], s=other_core)

    def over_x(k):
        return remote(own.at[k, mine], w_ref.at[k, x, core, mine], send.at[1, k], recv.at[1, k], s=other_x)

    def over_y(k):
        at = w_ref.at[k, 1 - x, core, mine]
        return remote(at, at, send.at[2, k], recv.at[2, k], r=other_y)

    def on_first(k):
        at = w_ref.at[k, 1 - x, core, mine]
        return remote(at, at, send.at[3, k], recv.at[3, k], s=other_core)

    def on_second(k):
        at = w_ref.at[k, 1 - x, core, theirs]
        return remote(at, at, send.at[4, k], recv.at[4, k], s=other_core)

    def kept(k):
        return pltpu.make_async_copy(own.at[k], w_ref.at[k, x, core], keep.at[k])

    def fetched(k, slot):
        return pltpu.make_async_copy(w_ref.at[k], wbuf.at[slot], fetch.at[slot])

    def from_x(k):
        over_x(k).wait_recv()
        over_y(k).start()
        on_first(k).start()

    def from_y(k):
        over_y(k).wait_recv()
        on_second(k).start()

    def whole(k):
        for copy in (over_core, on_first, on_second):
            copy(k).wait_recv()
        kept(k).wait()

    @pl.when(step == 0)
    def _():
        barrier = pltpu.get_barrier_semaphore()
        for to in ({"s": other_core}, {"s": other_x}, {"r": other_y}):
            pl.semaphore_signal(barrier, inc=1, device_id=to, device_id_type=MESH)
        rows, part = own.shape[1] // 3, own.shape[2] // 4
        for layer in range(2):
            down = d_ref[layer].T
            for chunk in range(CHUNKS):
                k = layer * CHUNKS + chunk
                for q in range(4):
                    to = slice(q * part, (q + 1) * part)
                    at = slice((q * CHUNKS + chunk) * part, (q * CHUNKS + chunk + 1) * part)
                    own[k, 0:rows, to] = g_ref[layer, :, at]
                    own[k, rows : 2 * rows, to] = u_ref[layer, :, at]
                    own[k, 2 * rows :, to] = down[q * rows : (q + 1) * rows, chunk * part : (chunk + 1) * part]
        pl.semaphore_wait(barrier, 3)

        @pl.loop(0, count)
        def _(k):
            over_x(k).start()
            over_core(k).start()
            kept(k).start()

        from_x(0)
        from_x(1)
        from_y(0)
        whole(0)
        fetched(0, 0).start()

    @pl.when((lax.rem(step, 2) == 1) & (step < 2 * count - 4))
    def _():
        from_x((step + 3) // 2)

    @pl.when((lax.rem(step, 2) == 1) & (step < 2 * count - 2))
    def _():
        from_y((step + 1) // 2)

    @pl.when((lax.rem(step, 2) == 0) & (step > 0))
    def _():
        whole(step // 2)

    @pl.when(t == 0)
    def _():
        slot = lax.rem(j, 2)
        fetched(j, slot).wait()
        unpack(wbuf.at[slot], wg, wu, wd)

    @pl.when((t == STEPS - 1) & (j < CHUNKS - 1))
    def _():
        fetched(j + 1, lax.rem(j + 1, 2)).start()

    @pl.when(j == 0)
    def _():
        wide, scale = normed(x_ref[...])
        a_s[t] = (wide * scale).astype(BF)
        out_s[t] = jnp.zeros_like(out_s[t])

    for i in range(TILE // WIDE):
        at = slice(i * WIDE, (i + 1) * WIDE)
        a = a_s[t, at, :]
        gate, up = dot(a, wg[...]), dot(a, wu[...])
        gate_ref[0, at, :] = gate
        up_ref[0, at, :] = up
        hidden = (gate * jax.nn.sigmoid(gate) * up).astype(BF)
        out_s[t, :, at] += dot(wd[...], hidden, NT)

    @pl.when(j == CHUNKS - 1)
    def _():
        h_ref[...] = x_ref[...] + out_s[t].astype(BF).T

    @pl.when(step == CHUNKS * STEPS - 1)
    def _():
        @pl.loop(0, count)
        def _(k):
            for copy in (over_core, over_x, over_y, on_first, on_second):
                copy(k).wait_send()


class Sum:
    def __init__(self, count, g_ref, p_s, r1, r2, z_s, ry, rz, g_s, keep, send, recv, credit):
        self.count, self.slots = count, p_s.shape[0]
        self.g, self.p_s, self.r1, self.r2, self.z_s, self.ry, self.rz, self.g_s = g_ref, p_s, r1, r2, z_s, ry, rz, g_s
        self.keep, self.send, self.recv, self.credit = keep, send, recv, credit
        self.r, self.x, self.y, self.core, self.other_y, self.other_x, self.other_core = place()
        self.z = lax.rem(self.r, 4)
        self.partners = [({"s": self.other_core}, 0), ({"s": self.other_x}, 1), ({"r": self.other_y}, 2)]
        self.partners += [({"r": self.along_z(d)}, 6 - d) for d in range(1, 4)]

    @staticmethod
    def scratch(slots, rows, width):
        piece = (rows // 2, width // 4)
        return [
            pltpu.VMEM((slots, 2, 2, rows, width), BF),
            pltpu.VMEM((slots, 2, rows, width), BF),
            pltpu.VMEM((slots, rows, width), BF),
            pltpu.VMEM((slots, 8) + piece, BF),
            pltpu.VMEM((slots, 4) + piece, BF),
            pltpu.VMEM((slots, 4) + piece, BF),
            pltpu.VMEM((slots, 8) + piece, BF),
            DMA((slots,)),
            DMA((slots, 17)),
            DMA((slots, 17)),
            pltpu.SemaphoreType.REGULAR((6,)),
        ]

    def along_z(self, d):
        return 4 * self.y + lax.rem(self.z + d, 4)

    def copy(self, src, dst, k, which, **to):
        return remote(src, dst, self.send.at[k % self.slots, which], self.recv.at[k % self.slots, which], **to)

    def over_core(self, k):
        n = k % self.slots
        return self.copy(self.p_s.at[n, :, 1 - self.core], self.r1.at[n], k, 0, s=self.other_core)

    def over_x(self, k, h):
        n = k % self.slots
        rows = self.rows(self.y if h else 1 - self.y)
        return self.copy(self.p_s.at[n, 1 - self.x, self.core, rows], self.r2.at[n, rows], k, 1 + h, s=self.other_x)

    def over_y(self, k, d):
        n, at = k % self.slots, lax.rem(self.z + d, 4)
        return self.copy(self.z_s.at[n, 4 * (1 - self.y) + at], self.ry.at[n, at], k, 3 + d, r=self.other_y)

    def over_z(self, k, d):
        n = k % self.slots
        return self.copy(self.z_s.at[n, self.along_z(d)], self.rz.at[n, self.z], k, 6 + d, r=self.along_z(d))

    def back_z(self, k, d):
        at = self.g_s.at[k % self.slots, self.r]
        return self.copy(at, at, k, 9 + d, r=self.along_z(d))

    def back_y(self, k, d):
        at = self.g_s.at[k % self.slots, self.along_z(d)]
        return self.copy(at, at, k, 13 + d, r=self.other_y)

    def rows(self, y):
        high = self.z_s.shape[2]
        return pl.ds(pl.multiple_of(y * high, high), high)

    def held(self, k, y, d):
        n, wide = k % self.slots, self.z_s.shape[3]
        at = (self.rows(y), pl.ds(pl.multiple_of(lax.rem(self.z + d, 4) * wide, wide), wide))
        parts = self.p_s[(n, self.x, self.core) + at], self.r1[(n, self.x) + at], self.r2[(n,) + at]
        return parts[0].astype(F32) + parts[1].astype(F32) + parts[2].astype(F32)

    def kept(self, k):
        return pltpu.make_async_copy(self.g_s.at[k % self.slots], self.g.at[k], self.keep.at[k % self.slots])

    def greet(self):
        barrier = pltpu.get_barrier_semaphore()
        for to, _ in self.partners:
            pl.semaphore_signal(barrier, inc=1, device_id=to, device_id_type=MESH)
        pl.semaphore_wait(barrier, 6)

    def begin(self, k):
        if k >= self.slots:
            for i in range(6):
                pl.semaphore_wait(self.credit.at[i], 1)
        self.over_core(k).start()

    def add_core(self, k):
        n, away = k % self.slots, 1 - self.x
        self.over_core(k).wait_recv()
        for h in range(2):
            rows = self.rows(self.y if h else 1 - self.y)
            both = self.p_s[n, away, self.core, rows].astype(F32) + self.r1[n, away, rows].astype(F32)
            self.p_s[n, away, self.core, rows] = both.astype(BF)
            self.over_x(k, h).start()

    def add_x(self, k):
        n, away = k % self.slots, 1 - self.y
        self.over_x(k, 0).wait_recv()
        for d in (1, 2, 3, 0):
            self.z_s[n, 4 * away + lax.rem(self.z + d, 4)] = self.held(k, away, d).astype(BF)
            self.over_y(k, d).start()

    def add_y(self, k):
        n = k % self.slots
        self.over_x(k, 1).wait_recv()
        for d in (1, 2, 3):
            self.over_y(k, d).wait_recv()
            self.z_s[n, self.along_z(d)] = (self.held(k, self.y, d) + self.ry[n, lax.rem(self.z + d, 4)].astype(F32)).astype(BF)
            self.over_z(k, d).start()

    def add_z(self, k):
        n = k % self.slots
        self.over_y(k, 0).wait_recv()
        total = self.held(k, self.y, 0) + self.ry[n, self.z].astype(F32)
        for d in range(1, 4):
            self.over_z(k, d).wait_recv()
        for d in range(1, 4):
            total += self.rz[n, lax.rem(self.z + d, 4)].astype(F32)
        self.g_s[n, self.r] = total.astype(BF)
        for d in range(1, 4):
            self.back_z(k, d).start()
        self.back_y(k, 0).start()

    def gather_y(self, k):
        for d in (1, 3, 2):
            self.back_z(k, 4 - d).wait_recv()
            self.back_y(k, d).start()

    def finish(self, k):
        for d in range(4):
            self.back_y(k, d).wait_recv()
        self.kept(k).start()
        self.over_core(k).wait_send()
        for h in range(2):
            self.over_x(k, h).wait_send()
        for d in range(4):
            self.over_y(k, d).wait_send()
            self.back_y(k, d).wait_send()
        for d in range(1, 4):
            self.over_z(k, d).wait_send()
            self.back_z(k, d).wait_send()

    def release(self, k):
        self.kept(k).wait()
        if k + self.slots < self.count:
            for to, i in self.partners:
                pl.semaphore_signal(self.credit.at[i], inc=1, device_id=to, device_id_type=MESH)

    def timed(self, begins, after):
        stages = (self.begin, self.add_core, self.add_x, self.add_y, self.add_z, self.gather_y, self.finish, self.release)
        return [(at + late, functools.partial(stage, k)) for k, at in enumerate(begins) for stage, late in zip(stages, (0,) + after, strict=True)]


EARLY = 3


def run_at(step, timed, last):
    timed = sorted(timed, key=lambda one: one[0])
    for at in sorted({one[0] for one in timed if one[0] <= last}):

        @pl.when(step == at)
        def _(at=at):
            for when, what in timed:
                if when == at:
                    what()

    return [what for when, what in timed if when > last]


def backward_kernel(first, h_ref, dy_ref, w_ref, *refs):
    if first:
        gate_ref, up_ref, q_ref, g_ref, at_s, dyt_s, dg_s, du_s, dd_s, wg, wu, wd, *scratch, load = refs
        total = Sum(2 * CHUNKS - EARLY, g_ref, *scratch)
    else:
        g_ref, q_ref, dh_ref, at_s, dyt_s, dg_s, du_s, dd_s, wg, wu, wd, a_s, da_s, *scratch, load = refs
        total = Sum(EARLY, g_ref, *scratch)
    j, t = pl.program_id(0), pl.program_id(1)
    step, last = j * STEPS + t, CHUNKS * STEPS - 1
    p_s, slots = total.p_s, total.slots

    if first:

        def taken(i):
            return pltpu.make_async_copy(q_ref.at[i], p_s.at[i], load.at[i])

        timed = [(0, taken(i).start) for i in range(CHUNKS - EARLY)] + [(0, total.greet)]
        timed += [(3 * i, taken(i).wait) for i in range(CHUNKS - EARLY)]
        timed += total.timed((0, 3, 6, 9, 12, 16, last + 0.9), (1, 4, 6, 8, 10, 11, 12))
        ahead = CHUNKS - EARLY
    else:

        def taken(i):
            return pltpu.make_async_copy(p_s.at[(EARLY + i) % slots], q_ref.at[i], load.at[i])

        timed = [(0, total.greet)] + total.timed((4, 8, 12), (1, 3, 4, 5, 6, 7, 7))
        timed += [(STEPS * (EARLY + i + 1), taken(i).start) for i in range(CHUNKS - EARLY)]
        timed += [(last + 2, taken(i).wait) for i in range(CHUNKS - EARLY)]
        ahead = 0
    rest = run_at(step, timed, last)

    @pl.when(t == 0)
    def _():
        unpack(w_ref.at[0], wg, wu, wd)
        for s in (dg_s, du_s, dd_s):
            s[...] = jnp.zeros_like(s)

    @pl.when(j == 0)
    def _():
        wide, scale = normed(h_ref[...])
        a = (wide * scale).astype(BF)
        at_s[t] = a.T
        dyt_s[t] = dy_ref[...].T
        if not first:
            a_s[t] = a
            da_s[t] = jnp.zeros_like(da_s[t])

    for i in range(TILE // SUB):
        at = slice(i * SUB, (i + 1) * SUB)
        if first:
            gate, up = gate_ref[0, at, :], up_ref[0, at, :]
        else:
            a = a_s[t, at, :]
            gate, up = dot(a, wg[...]), dot(a, wu[...])
        by_hidden = dot(dy_ref[at, :], wd[...]).astype(BF).astype(F32)
        sig = jax.nn.sigmoid(gate)
        silu = gate * sig
        hidden = (silu * up).astype(BF)
        by_up = (by_hidden * silu).astype(BF)
        by_gate = (by_hidden * up * (sig + silu * (1.0 - sig))).astype(BF)
        dd_s[...] += dot(dyt_s[t, :, at], hidden)
        du_s[...] += dot(at_s[t, :, at], by_up)
        dg_s[...] += dot(at_s[t, :, at], by_gate)
        if not first:
            da_s[t, :, at] += dot(wg[...], by_gate, NT) + dot(wu[...], by_up, NT)

    @pl.when(t == STEPS - 1)
    def _():
        pack(p_s.at[lax.rem(j + ahead, slots)], dg_s, du_s, dd_s)

    if not first:

        @pl.when(j == CHUNKS - 1)
        def _():
            wide, scale = normed(h_ref[...])
            da = da_s[t].astype(BF).T.astype(F32)
            inner = jnp.mean(da * wide, -1, keepdims=True)
            dh_ref[...] = dy_ref[...] + (da * scale - wide * (scale * scale * scale * inner)).astype(BF)

    @pl.when(step == last)
    def _():
        for what in rest:
            what()


def adamw(w, m, v, g):
    g = g.astype(F32)
    m = 0.9 * m + 0.1 * g
    v = 0.95 * v + 0.05 * g * g
    step = m * lax.rsqrt(v + 1e-8) + 0.1 * w.astype(F32)
    return (w.astype(F32) - 0.02 * step).astype(BF), m, v


def update_kernel(early, late, early_rows, late_rows, *refs):
    *refs, turned = refs
    rows = refs[0].shape[1]
    part = early.shape[-1]
    layer, s = pl.program_id(0), pl.program_id(1)
    skip = 2 * rows - early.shape[3]

    def take(columns, downs):
        for chunk, (g, n) in enumerate(columns):
            at = slice(chunk * part, (chunk + 1) * part)
            both = jnp.concatenate([g[n, 0, 0], g[n, 1, 0, :skip]], 0)
            for i in range(2):
                new = adamw(*(refs[3 * i + k][0, :, at] for k in range(3)), both[i * rows : (i + 1) * rows])
                for k in range(3):
                    refs[9 + 3 * i + k][0, :, at] = new[k]

        @pl.when(s == 0)
        def _():
            for chunk, (g, n) in enumerate(downs):
                turned[chunk * part : (chunk + 1) * part, :] = jnp.concatenate([g[n, 0, q, skip:] for q in range(4)], 0).T

    def chunks(low, high):
        return [(high, CHUNKS - EARLY + n) for n in range(CHUNKS)], [(low, n) for n in range(EARLY)] + [(high, n) for n in range(CHUNKS - EARLY)]

    for number in range(2):

        @pl.when(layer == number)
        def _(number=number):
            take(chunks(early, late)[number], chunks(early_rows, late_rows)[number])

    new = adamw(*(refs[6 + k][0] for k in range(3)), turned[pl.ds(pl.multiple_of(s * rows, rows), rows), :])
    for k in range(3):
        refs[15 + k][0] = new[k]


def solution(mesh):
    def step(x, dy, *arrays):
        x, dy = x[0], dy[0]
        weights, m, v = (arrays[i : i + 3] for i in (0, 3, 6))
        tokens, d = x.shape
        layers, rows, ff = weights[0].shape
        width, deep = ff // CHUNKS, 3 * rows
        part = width // 4
        shape = jax.ShapeDtypeStruct

        def params(flops, **more):
            return dict(
                compiler_params=pltpu.CompilerParams(vmem_limit_bytes=VMEM_LIMIT, **more),
                cost_estimate=pl.CostEstimate(flops=flops * tokens * d * ff, bytes_accessed=0, transcendentals=0),
            )

        tok = pl.BlockSpec((TILE, d), lambda j, t: (t, 0))
        late = pl.BlockSpec((TILE, d), lambda j, t: (jnp.where(j == CHUNKS - 1, t, 0), 0))
        saved = pl.BlockSpec((1, TILE, width), lambda j, t: (j, t, 0))
        package = pl.BlockSpec((1, 2, 2, deep, width), lambda j, t: (j, 0, 0, 0, 0))
        above = pl.BlockSpec((1, 2, 2, deep, width), lambda j, t: (CHUNKS + j, 0, 0, 0, 0))
        packages = shape((CHUNKS - EARLY, 2, 2, deep, width), BF)
        grads = [shape((n, 8, deep // 2, part), BF) for n in (EARLY, 2 * CHUNKS - EARLY)]
        matrices = [pltpu.VMEM((d, width), BF)] * 3
        across = [pltpu.VMEM((STEPS, d, TILE), BF)] * 2
        sums = [pltpu.VMEM((d, width), F32)] * 3
        count = layers * CHUNKS

        w, h, gate, up = pl.pallas_call(
            forward_kernel,
            grid=(CHUNKS, STEPS),
            in_specs=[pl.BlockSpec(w.shape, lambda j, t: (0, 0, 0), pipeline_mode=pl.Buffered(1)) for w in weights] + [tok],
            out_specs=[ANY, late, saved, saved],
            out_shape=[shape((count, 2, 2, deep, width), BF), shape(x.shape, BF)] + [shape((CHUNKS, tokens, width), F32)] * 2,
            scratch_shapes=[pltpu.VMEM((STEPS, TILE, d), BF), pltpu.VMEM((STEPS, d, TILE), F32)]
            + matrices
            + [pltpu.VMEM((count, deep, width), BF), pltpu.VMEM((2, 2, 2, deep, width), BF)]
            + [DMA((count,)), DMA((2,)), DMA((5, count)), DMA((5, count))],
            name="forward",
            **params(6, collective_id=0, has_side_effects=True),
        )(*weights, x)
        early, waiting, dh = pl.pallas_call(
            functools.partial(backward_kernel, False),
            grid=(CHUNKS, STEPS),
            in_specs=[tok, tok, above],
            out_specs=[ANY, ANY, late],
            out_shape=[grads[0], packages, shape(x.shape, BF)],
            scratch_shapes=across + sums + matrices + [pltpu.VMEM((STEPS, TILE, d), BF), pltpu.VMEM((STEPS, d, TILE), F32)] + Sum.scratch(2, deep, width) + [DMA((2,))],
            name="backward_1",
            **params(16, collective_id=1, has_side_effects=True),
        )(h, dy, w)
        rest = pl.pallas_call(
            functools.partial(backward_kernel, True),
            grid=(CHUNKS, STEPS),
            in_specs=[tok, tok, package, saved, saved, ANY],
            out_specs=ANY,
            out_shape=grads[1],
            scratch_shapes=across + sums + matrices + Sum.scratch(4, deep, width) + [DMA((2,))],
            name="backward_0",
            **params(8, collective_id=2, has_side_effects=True),
        )(x, dh, w, gate, up, waiting)

        g = [total.reshape(-1, 2, 4, deep // 2, part) for total in (early, rest)]
        block = pl.BlockSpec((1, rows, CHUNKS * part), lambda layer, s: (layer, 0, s))
        quarter = pl.BlockSpec((1, rows, d), lambda layer, s: (layer, s, 0))
        columns = [pl.BlockSpec((total.shape[0], 2, 1, deep // 2, part), lambda layer, s: (0, 0, s, 0, 0)) for total in g]
        downs = [pl.BlockSpec((total.shape[0], 1, 4, deep // 2, part), lambda layer, s: (0, 1, 0, 0, 0)) for total in g]
        blocks = [block] * 6 + [quarter] * 3
        new = pl.pallas_call(
            update_kernel,
            grid=(layers, 4),
            in_specs=columns + downs + blocks,
            out_specs=blocks,
            out_shape=[shape(weights[i].shape, t) for i in range(3) for t in (BF, F32, F32)],
            scratch_shapes=[pltpu.VMEM((CHUNKS * part, d), BF)],
            name="update",
            **params(1),
        )(*g, *g, *(one for i in range(3) for one in (weights[i], m[i], v[i])))
        return tuple(new[3 * i + k] for k in range(3) for i in range(3))

    states, cut = P(("rep", "r", "s"), None, None), P(None, "s", None)
    return jax.shard_map(step, mesh=mesh, in_specs=(states, states) + (cut,) * 9, out_specs=(P("rep", "s", None),) * 9, check_vma=False)
```
